32 devices in a mesh: feat: 8 (over z, y), row: 2 (over x), col: 2 (over core).
Axes of the slice: x: 2, y: 2, z: 4, core: 2. Of those that a mesh axis runs over, the one named last changes fastest.
Arguments:
- local_x: float32 [4, 32, 256], P(('row', 'col'), 'feat'), may hold values from -4 to 4
- dual_var: float32 [4, 32, 256], P(('row', 'col'), 'feat'), may hold values from -2 to 2
- consensus_old: float32 [32, 256], P('feat'), may hold values from -4 to 4
- blocks_data: bfloat16 [4, 32, 512, 256], P(('row', 'col'), 'feat'), may hold values from -0.375 to 0.375
- row_index: int32 [4, 32, 512], P(('row', 'col'), 'feat'), may hold values from 0 to 16383, as said below
- labels: int32 [4, 16384], P(('row', 'col')), may hold values 0 or 1
Outputs:
- solved_x: float32 [4, 32, 256], P(('row', 'col'), 'feat')
- dual_new: float32 [4, 32, 256], P(('row', 'col'), 'feat')
- consensus: float32 [32, 256], P('feat')
- norms: float32 [2], replicated
The draws below stay inside these ranges and needn't reach their ends.
Inputs may be any that keep to these rules, and one draw needn't show every extreme that they name: `row_index`: the 512 rows of one block are distinct samples of its shard; a sample may appear in no block or in several.
All inputs are finite; a program needn't handle non-finite values. No bound on the sum of `labels` on one device may be relied on, other than what follows from the above.
Results may differ from the reference program's by a relative error of at most 0.0019.
Values sent between devices are 32-bit elements; how exact they have to be, the bound alone decides.
A program may use at most 64 MiB of HBM per device.

```python
import jax
import jax.numpy as jnp
from jax import lax

BLOCK_COLS = 256
BLOCK_ROWS = 512
SAMPLES_DEV = 16384
NEWTON_STEPS = 2
CG_STEPS = 3
SHARDS = 4
BLOCKS = 32


def draw_row_index(key, part):
    keys = jax.random.split(jax.random.fold_in(key, 17), SHARDS * BLOCKS)

    def one_block(block_key):
        return jax.random.permutation(block_key, SAMPLES_DEV)[:BLOCK_ROWS].astype(jnp.int32)
    picks = lax.map(one_block, keys)
    return picks.reshape(SHARDS, BLOCKS, BLOCK_ROWS).astype(jnp.int32)


def draw_dual_var(key, part):
    inner = jax.random.fold_in(key, 29)
    position = jnp.arange(BLOCKS, dtype=jnp.float32) / jnp.float32(max(BLOCKS - 1, 1))
    scales = 0.05 * jnp.power(10.0, position)
    raw = jax.random.normal(inner, (SHARDS, BLOCKS, BLOCK_COLS), jnp.float32)
    values = raw * scales[None, :, None]
    return jnp.clip(values, -2.0, 2.0).astype(jnp.float32)


def with_ends(drawn, key, low, largest):
    longest = drawn.shape.index(max(drawn.shape))
    spots = []
    for shift in (0, 1):
        where = [jax.random.randint(jax.random.fold_in(key, axis), (), 0, length) for axis, length in enumerate(drawn.shape)]
        where[longest] = (where[longest] + shift) % drawn.shape[longest]
        spots.append(tuple(where))
    return drawn.at[spots[0]].set(low).at[spots[1]].set(largest)


def levels(rng, extent, cuts, smallest, high):
    def one(dim, shards_of):
        draws = jax.random.uniform(jax.random.fold_in(jax.random.fold_in(rng, 6), dim), (shards_of,), jnp.float32, smallest / len(cuts), high / len(cuts))
        return jnp.repeat(jnp.exp(draws), extent[dim] // shards_of).reshape((-1,) + (1,) * (len(extent) - dim - 1))

    gain = one(*cuts[0])
    for cut in cuts[1:]:
        gain = gain * one(*cut)
    return gain


def bell_draw(key, extent, deviation, limit, cuts=(), kind=jnp.bfloat16):
    loudness = levels(key, extent, cuts, -0.22, 0.18) if cuts else 1.0
    drawn = jax.random.normal(key, extent, jnp.float32) * deviation * loudness
    return jnp.minimum(jnp.maximum(drawn, -limit), limit).astype(kind)


def setup_inputs(seed: int = 0) -> dict:
    arg_keys = jax.random.split(jax.random.key(seed), 7)
    local_x = bell_draw(arg_keys[0], (SHARDS, BLOCKS, BLOCK_COLS), 0.5, 4.0, ((0, 4), (1, 8)), jnp.float32)
    dual_var = draw_dual_var(jax.random.fold_in(arg_keys[6], 71), 0)
    consensus_old = bell_draw(arg_keys[2], (BLOCKS, BLOCK_COLS), 0.5, 4.0, ((0, 8),), jnp.float32)
    blocks_data = bell_draw(arg_keys[3], (SHARDS, BLOCKS, BLOCK_ROWS, BLOCK_COLS), BLOCK_COLS ** -0.5, 0.375, ((0, 4), (1, 8)))
    row_index = draw_row_index(jax.random.fold_in(arg_keys[6], 71), 0)
    labels = with_ends((jax.random.randint(arg_keys[5], (SHARDS, SAMPLES_DEV), 0, 2) < 1).astype(jnp.int32), jax.random.fold_in(arg_keys[5], 1), 0, 1)
    return {"local_x": local_x, "dual_var": dual_var, "consensus_old": consensus_old, "blocks_data": blocks_data, "row_index": row_index, "labels": labels}


penalty = 1.0
damping = 0.5
threshold = 0.05

def conjugate_solve(hessian, gradient):
    delta = jnp.zeros_like(gradient)
    residual = gradient
    direction = gradient
    power = lax.optimization_barrier(jnp.sum(residual * residual, axis=1))
    for cg_step in range(CG_STEPS):
        image = jnp.einsum('bkl,bl->bk', hessian, direction, precision=lax.Precision.HIGHEST)
        alpha = power / lax.optimization_barrier(jnp.sum(direction * image, axis=1))
        delta = delta + alpha[:, None] * direction
        residual = residual - alpha[:, None] * image
        power_next = lax.optimization_barrier(jnp.sum(residual * residual, axis=1))
        direction = residual + (power_next / power)[:, None] * direction
        power = power_next
    return delta

def newton_solve(iterate, blocks_data, row_index, labels, target):
    targets = labels.astype(jnp.float32)
    data_wide = blocks_data.astype(jnp.float32)
    flat_index = row_index.reshape(-1)
    identity = jnp.eye(iterate.shape[1], dtype=jnp.float32)
    for newton_step in range(NEWTON_STEPS):
        rounded = lax.optimization_barrier(iterate.astype(jnp.bfloat16)).astype(jnp.float32)
        partial_value = jnp.einsum('brk,bk->br', data_wide, rounded, precision=lax.Precision.HIGHEST)
        margins = jax.ops.segment_sum(partial_value.reshape(-1), flat_index, num_segments=SAMPLES_DEV)
        prob = jax.nn.sigmoid(margins)
        misfit = prob - targets
        weights = prob * (1.0 - prob)
        misfit_rows = lax.optimization_barrier(misfit[row_index].astype(jnp.bfloat16)).astype(jnp.float32)
        gradient = jnp.einsum('brk,br->bk', data_wide, misfit_rows, precision=lax.Precision.HIGHEST)
        gradient = gradient + penalty * (iterate - target)
        weighted = lax.optimization_barrier((data_wide * weights[row_index][:, :, None]).astype(jnp.bfloat16)).astype(jnp.float32)
        hessian = jnp.einsum('brk,brl->bkl', data_wide, weighted, precision=lax.Precision.HIGHEST) + penalty * identity
        delta = conjugate_solve(hessian, gradient)
        iterate = iterate - damping * delta
    return iterate

def reference(local_x, dual_var, consensus_old, blocks_data, row_index, labels):
    shards = jnp.float32(local_x.shape[0])

    def one_shard(items):
        return newton_solve(items[0], items[1], items[2], items[3], consensus_old - items[4])
    solved = lax.map(one_shard, (local_x, blocks_data, row_index, labels, dual_var))
    averaged = lax.optimization_barrier(jnp.sum(solved + dual_var, axis=0)) / shards
    consensus = jnp.sign(averaged) * jnp.maximum(jnp.abs(averaged) - threshold, 0.0)
    dual_new = dual_var + solved - consensus
    primal = jnp.sqrt(jnp.sum((solved - consensus) ** 2))
    dual_norm = penalty * jnp.sqrt(shards * jnp.sum((consensus - consensus_old) ** 2))
    return (solved, dual_new, consensus, jnp.stack([primal, dual_norm]))
```

```python
import functools

import jax
import jax.numpy as jnp
from jax import lax
from jax.experimental import pallas as pl
from jax.experimental.pallas import tpu as pltpu
from jax.sharding import PartitionSpec as P

NEWTON_STEPS = 2
CG_STEPS = 3

penalty = 1.0
damping = 0.5
threshold = 0.05

MESH = pl.DeviceIdType.MESH
F32 = jnp.float32
BF16 = jnp.bfloat16
LANES = 128


def dot_nt(a, b):
    return lax.dot_general(a, b, (((1,), (1,)), ((), ())), preferred_element_type=F32)


def dot_nn(a, b):
    return lax.dot_general(a, b, (((1,), (0,)), ((), ())), preferred_element_type=F32)


def two_terms(value):
    high = value.astype(BF16).astype(F32)
    return high, value - high


def stacked(value):
    return jnp.concatenate(two_terms(value), axis=0).astype(BF16)


def kernel(
    n, rows, cols,
    lx, dual, cons, idx, lab, data_hbm,
    sx_out, dn_out, co_out, norm_out,
    data, p_all, idx_all, fin, nrm, oh_hi, oh_lo,
    data_sem, idx_ss, idx_rs, p_ss, p_rs, fin_ss, fin_rs, nrm_ss, nrm_rs,
):
    shards = rows * cols
    _, blocks, height, width = data_hbm.shape
    high_size = lab.shape[0]
    me = lax.axis_index("feat")
    shard = lax.axis_index("row") * cols + lax.axis_index("col")

    load = pltpu.make_async_copy(data_hbm.at[0], data, data_sem)
    load.start()

    barrier = pltpu.get_barrier_semaphore()

    def shard_id(other):
        return {"row": other // cols, "col": other % cols}

    @pl.loop(1, n)
    def _(k):
        pl.semaphore_signal(
            barrier, inc=1, device_id={"feat": (me + k) % n}, device_id_type=MESH)

    for j in range(1, shards):
        pl.semaphore_signal(
            barrier, inc=1, device_id=shard_id((shard + j) % shards), device_id_type=MESH)

    def feat_copy(src, dst, send, recv, target):
        return pltpu.make_async_remote_copy(
            src_ref=src, dst_ref=dst, send_sem=send, recv_sem=recv,
            device_id={"feat": target}, device_id_type=MESH)

    def sends(src, dst, send, recv):
        @pl.loop(1, n)
        def _(k):
            feat_copy(src, dst.at[me], send.at[k], recv.at[me], (me + k) % n).start()

    def wait_from(src, dst, send, recv, k):
        source = (me + n - k) % n
        feat_copy(src, dst.at[source], send.at[k], recv.at[source], (me + k) % n).wait_recv()
        return source

    def wait_sends(src, dst, send, recv):
        @pl.loop(1, n)
        def _(k):
            feat_copy(src, dst.at[me], send.at[k], recv.at[me], (me + k) % n).wait_send()

    def one_hot(index_row, size):
        lane = lax.broadcasted_iota(jnp.int32, (size, height), 0)
        return lane == index_row

    own = idx[0]
    labels_hl = lab[...].astype(F32).astype(BF16)
    targets = []
    for b in range(blocks):
        row = own[b:b + 1, :]
        high = one_hot(row // LANES, high_size).astype(F32)
        low = one_hot(row % LANES, LANES).astype(F32)
        oh_hi[b] = high.astype(BF16)
        oh_lo[b] = low.astype(BF16)
        picked = dot_nn(labels_hl, low.astype(BF16))
        targets.append(jnp.sum(picked * high, axis=0, keepdims=True))

    pl.semaphore_wait(barrier, n - 1 + shards - 1)
    sends(idx.at[0], idx_all, idx_ss, idx_rs)

    iterate = lx[0]
    dual_local = dual[0]
    target = cons[...] - dual_local
    load.wait()
    flat = data[...].reshape(blocks * height, width)
    block_of = lax.broadcasted_iota(jnp.int32, (blocks, height), 0)

    def place(pieces):
        return jnp.concatenate(
            [jnp.where(block_of == b, pieces[b], 0.0) for b in range(blocks)], axis=1)

    def scatter(index, values):
        total = jnp.zeros((LANES, 2 * high_size), F32)
        first, second = two_terms(values)
        for b in range(blocks):
            row = index[b:b + 1, :]
            mask = one_hot(row // LANES, high_size)
            low = one_hot(row % LANES, LANES).astype(F32).astype(BF16)
            spread = jnp.concatenate(
                [jnp.where(mask, first[b:b + 1, :], 0.0).astype(BF16),
                 jnp.where(mask, second[b:b + 1, :], 0.0).astype(BF16)], axis=0)
            total += dot_nt(low, spread)
        return total

    for step in range(NEWTON_STEPS):
        slots = p_all.at[step]
        products = dot_nt(iterate.astype(BF16), flat)
        partial_value = jnp.concatenate(
            [products[b:b + 1, b * height:(b + 1) * height] for b in range(blocks)], axis=0)
        slots[me] = partial_value
        sends(slots.at[me], slots, p_ss.at[step], p_rs.at[step])
        total = scatter(own, partial_value)

        def collect(k, total):
            if step == 0:
                wait_from(idx.at[0], idx_all, idx_ss, idx_rs, k)
            source = wait_from(slots.at[me], slots, p_ss.at[step], p_rs.at[step], k)
            return total + scatter(idx_all[source], slots[source])

        total = lax.fori_loop(1, n, collect, total)
        margins_t = total[:, :high_size] + total[:, high_size:]
        margins_two = stacked(margins_t)
        misfit, weights = [], []
        for b in range(blocks):
            picked = dot_nn(margins_two, oh_hi[b])
            both = picked[:LANES] + picked[LANES:]
            margin = jnp.sum(both * oh_lo[b].astype(F32), axis=0, keepdims=True)
            prob = 1.0 / (1.0 + jnp.exp(-margin))
            misfit.append(prob - targets[b])
            weights.append(prob * (1.0 - prob))
        weight_place = place(weights)
        gradient = dot_nn(place(misfit).astype(BF16), flat) + penalty * (iterate - target)

        delta = jnp.zeros_like(gradient)
        residual = gradient
        direction = gradient
        power = jnp.sum(residual * residual, axis=1, keepdims=True)
        for cg_step in range(CG_STEPS):
            product = dot_nt(stacked(direction), flat)
            scaled = (product[:blocks] + product[blocks:]) * weight_place
            image = dot_nn(stacked(scaled), flat)
            image = image[:blocks] + image[blocks:] + penalty * direction
            alpha = power / jnp.sum(direction * image, axis=1, keepdims=True)
            delta = delta + alpha * direction
            if cg_step < CG_STEPS - 1:
                residual = residual - alpha * image
                power_next = jnp.sum(residual * residual, axis=1, keepdims=True)
                direction = residual + (power_next / power) * direction
                power = power_next
        iterate = iterate - damping * delta

    fin[shard, 0] = iterate + dual_local
    fin[shard, 1] = iterate

    def fin_copy(j, slot):
        return pltpu.make_async_remote_copy(
            src_ref=fin.at[shard], dst_ref=fin.at[slot],
            send_sem=fin_ss.at[j], recv_sem=fin_rs.at[slot],
            device_id=shard_id((shard + j) % shards), device_id_type=MESH)

    for j in range(1, shards):
        fin_copy(j, shard).start()
    for j in range(1, shards):
        fin_copy(j, (shard + shards - j) % shards).wait_recv()
    totals = fin[0, 0]
    for s in range(1, shards):
        totals += fin[s, 0]
    averaged = totals / F32(shards)
    size = jnp.maximum(jnp.abs(averaged) - threshold, 0.0)
    consensus = jnp.where(averaged > 0.0, size, -size)
    change = (consensus - cons[...]) ** 2
    primal = (fin[0, 1] - consensus) ** 2
    for s in range(1, shards):
        primal += (fin[s, 1] - consensus) ** 2
    nrm[me] = jnp.concatenate(
        [jnp.sum(primal, axis=0, keepdims=True), jnp.sum(change, axis=0, keepdims=True)], axis=0)
    sends(nrm.at[me], nrm, nrm_ss, nrm_rs)
    sx_out[0] = iterate
    dn_out[0] = dual_local + iterate - consensus
    co_out[...] = consensus
    for j in range(1, shards):
        fin_copy(j, shard).wait_send()
    wait_sends(idx.at[0], idx_all, idx_ss, idx_rs)
    for step in range(NEWTON_STEPS):
        slots = p_all.at[step]
        wait_sends(slots.at[me], slots, p_ss.at[step], p_rs.at[step])

    @pl.loop(1, n)
    def _(k):
        wait_from(nrm.at[me], nrm, nrm_ss, nrm_rs, k)

    sums = jnp.sum(jnp.sum(nrm[...], axis=0), axis=1, keepdims=True)
    factor = lax.broadcasted_iota(jnp.int32, sums.shape, 0)
    scaled = jnp.where(factor == 0, sums, F32(shards) * sums)
    norms = jnp.sqrt(scaled) * jnp.where(factor == 0, 1.0, penalty)
    norm_out[0] = norms[0, 0]
    norm_out[1] = norms[1, 0]
    wait_sends(nrm.at[me], nrm, nrm_ss, nrm_rs)


def local(mesh, local_x, dual_var, consensus_old, blocks_data, row_index, labels):
    n, rows, cols = mesh.shape["feat"], mesh.shape["row"], mesh.shape["col"]
    shards = rows * cols
    _, blocks, height, width = blocks_data.shape
    samples = labels.shape[1]
    high_size = samples // LANES
    dma = pltpu.SemaphoreType.DMA
    vmem = pl.BlockSpec(memory_space=pltpu.VMEM)
    return pl.pallas_call(
        functools.partial(kernel, n, rows, cols),
        out_shape=(
            jax.ShapeDtypeStruct(local_x.shape, F32),
            jax.ShapeDtypeStruct(local_x.shape, F32),
            jax.ShapeDtypeStruct(consensus_old.shape, F32),
            jax.ShapeDtypeStruct((2,), F32),
        ),
        in_specs=[vmem] * 5 + [pl.BlockSpec(memory_space=pl.ANY)],
        out_specs=(vmem, vmem, vmem, pl.BlockSpec(memory_space=pltpu.SMEM)),
        scratch_shapes=[
            pltpu.VMEM((blocks, height, width), BF16),
            pltpu.VMEM((NEWTON_STEPS, n, blocks, height), F32),
            pltpu.VMEM((n, blocks, height), jnp.int32),
            pltpu.VMEM((shards, 2, blocks, width), F32),
            pltpu.VMEM((n, 2, width), F32),
            pltpu.VMEM((blocks, high_size, height), BF16),
            pltpu.VMEM((blocks, LANES, height), BF16),
            dma,
            dma((n,)), dma((n,)),
            dma((NEWTON_STEPS, n)), dma((NEWTON_STEPS, n)),
            dma((shards,)), dma((shards,)),
            dma((n,)), dma((n,)),
        ],
        compiler_params=pltpu.CompilerParams(
            collective_id=0, has_side_effects=True, vmem_limit_bytes=56 * 1024 * 1024),
        name="admm",
    )(local_x, dual_var, consensus_old, row_index, labels.reshape(high_size, LANES), blocks_data)


def solution(mesh):
    placed = (
        P(("row", "col"), "feat", None),
        P(("row", "col"), "feat", None),
        P("feat", None),
        P(("row", "col"), "feat", None, None),
        P(("row", "col"), "feat", None),
        P(("row", "col"), None),
    )
    return jax.shard_map(
        functools.partial(local, mesh),
        mesh=mesh,
        in_specs=placed,
        out_specs=(
            P(("row", "col"), "feat", None),
            P(("row", "col"), "feat", None),
            P("feat", None),
            P(),
        ),
        check_vma=False,
    )
```

```python
import functools

import jax
import jax.numpy as jnp
from jax import lax
from jax.experimental import pallas as pl
from jax.experimental.pallas import tpu as pltpu
from jax.sharding import PartitionSpec as P

NEWTON_STEPS = 2
CG_STEPS = 3

penalty = 1.0
damping = 0.5
threshold = 0.05

MESH = pl.DeviceIdType.MESH
F32 = jnp.float32
BF16 = jnp.bfloat16
LANE_BITS = 7
LANES = 1 << LANE_BITS


def dot_nt(a, b):
    return lax.dot_general(a, b, (((1,), (1,)), ((), ())), preferred_element_type=F32)


def dot_nn(a, b):
    return lax.dot_general(a, b, (((1,), (0,)), ((), ())), preferred_element_type=F32)


def two_terms(value):
    high = value.astype(BF16).astype(F32)
    return high, value - high


def kernel(
    n, rows, cols,
    lx_hbm, dual_hbm, cons_hbm, idx_hbm, lab_hbm, data_hbm,
    packed_out,
    lx, dual, cons, lab, data, data_t, hess, p_all, idx_all, fin, nrm, oh_hi, oh_lo,
    in_sem, idx_ss, idx_rs, p_ss, p_rs, fin_ss, fin_rs, nrm_ss, nrm_rs,
):
    shards = rows * cols
    blocks, height, width = data.shape
    high_size = lab.shape[0]
    me = lax.axis_index("feat")
    shard = lax.axis_index("row") * cols + lax.axis_index("col")

    loads = [
        pltpu.make_async_copy(source, place, in_sem.at[i])
        for i, (source, place) in enumerate([
            (idx_hbm.at[0], idx_all.at[me]),
            (data_hbm.at[0], data),
            (lab_hbm, lab),
            (lx_hbm.at[0], lx),
            (dual_hbm.at[0], dual),
            (cons_hbm, cons),
        ])
    ]
    for load in loads:
        load.start()

    barrier = pltpu.get_barrier_semaphore()

    def shard_id(other):
        return {"row": other // cols, "col": other % cols}

    @pl.loop(1, n)
    def _(k):
        pl.semaphore_signal(
            barrier, inc=1, device_id={"feat": (me + k) % n}, device_id_type=MESH)

    for j in range(1, shards):
        pl.semaphore_signal(
            barrier, inc=1, device_id=shard_id((shard + j) % shards), device_id_type=MESH)

    def feat_copy(src, dst, send, recv, target):
        return pltpu.make_async_remote_copy(
            src_ref=src, dst_ref=dst, send_sem=send, recv_sem=recv,
            device_id={"feat": target}, device_id_type=MESH)

    def sends(dst, send, recv):
        @pl.loop(1, n)
        def _(k):
            feat_copy(dst.at[me], dst.at[me], send.at[k], recv.at[me], (me + k) % n).start()

    def wait_from(dst, send, recv, k):
        source = (me + n - k) % n
        feat_copy(
            dst.at[source], dst.at[source], send.at[k], recv.at[source], (me + k) % n).wait_recv()
        return source

    def wait_sends(dst, send, recv):
        @pl.loop(1, n)
        def _(k):
            feat_copy(
                dst.at[me], dst.at[me], send.at[k], recv.at[me], (me + k) % n).wait_send()

    def hits(index_row, size):
        level = lax.broadcasted_iota(jnp.int32, (size, height), 0).astype(F32).astype(BF16)
        return level == index_row.astype(F32).astype(BF16)

    def high_hits(index_row):
        return hits(index_row >> LANE_BITS, high_size)

    def low_hits(index_row):
        return hits(index_row & (LANES - 1), LANES)

    one, zero = jnp.ones((), BF16), jnp.zeros((), BF16)

    for load in loads:
        load.wait()
    iterate = lx[...]
    dual_local = dual[...]
    target = cons[...] - dual_local

    own = idx_all[me]
    labels_hl = lab[...].astype(F32).astype(BF16)
    targets = []
    for b in range(blocks):
        row = own[b:b + 1, :]
        low = jnp.where(low_hits(row), one, zero)
        high = jnp.where(high_hits(row), one, zero)
        oh_hi[b] = high
        oh_lo[b] = low
        picked = dot_nn(labels_hl, low)
        targets.append(jnp.sum(picked * high.astype(F32), axis=0, keepdims=True))
        data_t[b] = data[b].T

    def products(iterate):
        rounded = iterate.astype(BF16)
        return jnp.concatenate(
            [dot_nn(rounded, data_t[b])[b:b + 1] for b in range(blocks)], axis=0)

    partial_value = products(iterate)
    p_all[0, me] = partial_value

    pl.semaphore_wait(barrier, n - 1 + shards - 1)
    sends(idx_all, idx_ss, idx_rs)

    def scatter(index, values):
        total = jnp.zeros((2 * high_size, LANES), F32)
        first, second = two_terms(values)
        first, second = first.astype(BF16), second.astype(BF16)
        for b in range(blocks):
            row = index[b:b + 1, :]
            mask = high_hits(row)
            low = jnp.where(low_hits(row), one, zero)
            spread = jnp.concatenate(
                [jnp.where(mask, first[b:b + 1, :], zero),
                 jnp.where(mask, second[b:b + 1, :], zero)], axis=0)
            total += dot_nt(spread, low)
        return total

    for step in range(NEWTON_STEPS):
        slots = p_all.at[step]
        if step > 0:
            partial_value = products(iterate)
            slots[me] = partial_value
        sends(slots, p_ss.at[step], p_rs.at[step])
        total = scatter(own, partial_value)

        def collect(k, total):
            if step == 0:
                wait_from(idx_all, idx_ss, idx_rs, k)
            source = wait_from(slots, p_ss.at[step], p_rs.at[step], k)
            return total + scatter(idx_all[source], slots[source])

        total = lax.fori_loop(1, n, collect, total)
        margins = total[:high_size] + total[high_size:]
        margins_two = jnp.concatenate(two_terms(margins), axis=0).astype(BF16)
        gradient = []
        for b in range(blocks):
            picked = dot_nn(margins_two, oh_lo[b])
            both = picked[:high_size] + picked[high_size:]
            margin = jnp.sum(both * oh_hi[b].astype(F32), axis=0, keepdims=True)
            prob = 1.0 / (1.0 + jnp.exp(-margin))
            weights = prob * (1.0 - prob)
            misfit = jnp.broadcast_to(prob - targets[b], (16, height))
            left = jnp.concatenate(
                [(data_t[b].astype(F32) * weights).astype(BF16), misfit.astype(BF16)], axis=0)
            made = dot_nn(left, data[b])
            hess[b] = made[:width]
            gradient.append(made[width:width + 1])
        gradient = jnp.concatenate(gradient, axis=0) + penalty * (iterate - target)

        delta = jnp.zeros_like(gradient)
        residual = gradient
        direction = gradient
        power = jnp.sum(residual * residual, axis=1, keepdims=True)
        for cg_step in range(CG_STEPS):
            turned = direction.T
            image = jnp.concatenate(
                [jnp.sum(hess[b] * turned[:, b:b + 1], axis=0, keepdims=True)
                 for b in range(blocks)], axis=0) + penalty * direction
            alpha = power / jnp.sum(direction * image, axis=1, keepdims=True)
            delta = delta + alpha * direction
            if cg_step < CG_STEPS - 1:
                residual = residual - alpha * image
                power_next = jnp.sum(residual * residual, axis=1, keepdims=True)
                direction = residual + (power_next / power) * direction
                power = power_next
        iterate = iterate - damping * delta

    fin[shard, 0] = iterate + dual_local
    fin[shard, 1] = iterate

    def fin_copy(j, slot):
        return pltpu.make_async_remote_copy(
            src_ref=fin.at[shard], dst_ref=fin.at[slot],
            send_sem=fin_ss.at[j], recv_sem=fin_rs.at[slot],
            device_id=shard_id((shard + j) % shards), device_id_type=MESH)

    for j in range(1, shards):
        fin_copy(j, shard).start()
    for j in range(1, shards):
        fin_copy(j, (shard + shards - j) % shards).wait_recv()
    totals = fin[0, 0]
    for s in range(1, shards):
        totals += fin[s, 0]
    averaged = totals / F32(shards)
    size = jnp.maximum(jnp.abs(averaged) - threshold, 0.0)
    consensus = jnp.where(averaged > 0.0, size, -size)
    change = (consensus - cons[...]) ** 2
    primal = (fin[0, 1] - consensus) ** 2
    for s in range(1, shards):
        primal += (fin[s, 1] - consensus) ** 2
    nrm[me] = jnp.concatenate(
        [jnp.sum(primal, axis=0, keepdims=True), jnp.sum(change, axis=0, keepdims=True)], axis=0)
    sends(nrm, nrm_ss, nrm_rs)
    packed_out[0] = iterate
    packed_out[1] = dual_local + iterate - consensus
    packed_out[2] = consensus
    for j in range(1, shards):
        fin_copy(j, shard).wait_send()
    wait_sends(idx_all, idx_ss, idx_rs)
    for step in range(NEWTON_STEPS):
        wait_sends(p_all.at[step], p_ss.at[step], p_rs.at[step])

    @pl.loop(1, n)
    def _(k):
        wait_from(nrm, nrm_ss, nrm_rs, k)

    sums = jnp.sum(jnp.sum(nrm[...], axis=0), axis=1, keepdims=True)
    factor = lax.broadcasted_iota(jnp.int32, sums.shape, 0)
    scaled = jnp.where(factor == 0, sums, F32(shards) * sums)
    norms = jnp.sqrt(scaled) * jnp.where(factor == 0, 1.0, penalty)
    packed_out[3, :2] = jnp.broadcast_to(norms, (2, width))
    wait_sends(nrm, nrm_ss, nrm_rs)


def unpack(packed, sx_out, dn_out, co_out, norm_out):
    sx_out[0] = packed[0]
    dn_out[0] = packed[1]
    co_out[...] = packed[2]
    norm_out[0] = packed[3, 0, 0]
    norm_out[1] = packed[3, 1, 0]


def local(mesh, local_x, dual_var, consensus_old, blocks_data, row_index, labels):
    n, rows, cols = mesh.shape["feat"], mesh.shape["row"], mesh.shape["col"]
    shards = rows * cols
    _, blocks, height, width = blocks_data.shape
    samples = labels.shape[1]
    high_size = samples // LANES
    dma = pltpu.SemaphoreType.DMA
    vmem = pl.BlockSpec(memory_space=pltpu.VMEM)
    packed = pl.pallas_call(
        functools.partial(kernel, n, rows, cols),
        out_shape=jax.ShapeDtypeStruct((4, max(blocks, 2), width), F32),
        in_specs=[pl.BlockSpec(memory_space=pl.ANY)] * 6,
        out_specs=vmem,
        scratch_shapes=[
            pltpu.VMEM((blocks, width), F32),
            pltpu.VMEM((blocks, width), F32),
            pltpu.VMEM((blocks, width), F32),
            pltpu.VMEM((high_size, LANES), jnp.int32),
            pltpu.VMEM((blocks, height, width), BF16),
            pltpu.VMEM((blocks, width, height), BF16),
            pltpu.VMEM((blocks, width, width), F32),
            pltpu.VMEM((NEWTON_STEPS, n, blocks, height), F32),
            pltpu.VMEM((n, blocks, height), jnp.int32),
            pltpu.VMEM((shards, 2, blocks, width), F32),
            pltpu.VMEM((n, 2, width), F32),
            pltpu.VMEM((blocks, high_size, height), BF16),
            pltpu.VMEM((blocks, LANES, height), BF16),
            dma((6,)),
            dma((n,)), dma((n,)),
            dma((NEWTON_STEPS, n)), dma((NEWTON_STEPS, n)),
            dma((shards,)), dma((shards,)),
            dma((n,)), dma((n,)),
        ],
        compiler_params=pltpu.CompilerParams(
            collective_id=0, has_side_effects=True, vmem_limit_bytes=56 * 1024 * 1024),
        name="admm",
    )(local_x, dual_var, consensus_old, row_index, labels.reshape(high_size, LANES), blocks_data)
    return pl.pallas_call(
        unpack,
        out_shape=(
            jax.ShapeDtypeStruct(local_x.shape, F32),
            jax.ShapeDtypeStruct(local_x.shape, F32),
            jax.ShapeDtypeStruct(consensus_old.shape, F32),
            jax.ShapeDtypeStruct((2,), F32),
        ),
        in_specs=[vmem],
        out_specs=(vmem, vmem, vmem, pl.BlockSpec(memory_space=pltpu.SMEM)),
        name="unpack",
    )(packed)


def solution(mesh):
    placed = (
        P(("row", "col"), "feat", None),
        P(("row", "col"), "feat", None),
        P("feat", None),
        P(("row", "col"), "feat", None, None),
        P(("row", "col"), "feat", None),
        P(("row", "col"), None),
    )
    return jax.shard_map(
        functools.partial(local, mesh),
        mesh=mesh,
        in_specs=placed,
        out_specs=(
            P(("row", "col"), "feat", None),
            P(("row", "col"), "feat", None),
            P("feat", None),
            P(),
        ),
        check_vma=False,
    )
```

```python
import functools

import jax
import jax.numpy as jnp
from jax import lax
from jax.experimental import pallas as pl
from jax.experimental.pallas import tpu as pltpu
from jax.sharding import PartitionSpec as P

NEWTON_STEPS = 2
CG_STEPS = 3

penalty = 1.0
damping = 0.5
threshold = 0.05

MESH = pl.DeviceIdType.MESH
F32 = jnp.float32
BF16 = jnp.bfloat16
LANE_BITS = 7
LANES = 1 << LANE_BITS


def dot_nt(a, b):
    return lax.dot_general(a, b, (((1,), (1,)), ((), ())), preferred_element_type=F32)


def dot_nn(a, b):
    return lax.dot_general(a, b, (((1,), (0,)), ((), ())), preferred_element_type=F32)


def two_terms(value):
    high = value.astype(BF16).astype(F32)
    return high, value - high


def kernel(
    n, rows, cols,
    lx_hbm, dual_hbm, cons_hbm, idx_hbm, lab_hbm, data_hbm,
    packed_out,
    lx, dual, cons, lab, data, data_t, hess, p_all, idx_all, fin, nrm, oh_hi, oh_lo,
    in_sem, idx_ss, idx_rs, p_ss, p_rs, fin_ss, fin_rs, nrm_ss, nrm_rs,
):
    shards = rows * cols
    blocks, height, width = data.shape
    high_size = lab.shape[0]
    me = lax.axis_index("feat")
    shard = lax.axis_index("row") * cols + lax.axis_index("col")

    loads = [
        pltpu.make_async_copy(source, place, in_sem.at[i])
        for i, (source, place) in enumerate([
            (idx_hbm.at[0], idx_all.at[me]),
            (data_hbm.at[0], data),
            (lab_hbm, lab),
            (lx_hbm.at[0], lx),
            (dual_hbm.at[0], dual),
            (cons_hbm, cons),
        ])
    ]
    for load in loads:
        load.start()

    barrier = pltpu.get_barrier_semaphore()

    def shard_id(other):
        return {"row": other // cols, "col": other % cols}

    @pl.loop(1, n)
    def _(k):
        pl.semaphore_signal(
            barrier, inc=1, device_id={"feat": (me + k) % n}, device_id_type=MESH)

    for j in range(1, shards):
        pl.semaphore_signal(
            barrier, inc=1, device_id=shard_id((shard + j) % shards), device_id_type=MESH)

    def feat_copy(src, dst, send, recv, target):
        return pltpu.make_async_remote_copy(
            src_ref=src, dst_ref=dst, send_sem=send, recv_sem=recv,
            device_id={"feat": target}, device_id_type=MESH)

    def sends(dst, send, recv):
        @pl.loop(1, n)
        def _(k):
            feat_copy(dst.at[me], dst.at[me], send.at[k], recv.at[me], (me + k) % n).start()

    def wait_from(dst, send, recv, k):
        source = (me + n - k) % n
        feat_copy(
            dst.at[source], dst.at[source], send.at[k], recv.at[source], (me + k) % n).wait_recv()
        return source

    def wait_sends(dst, send, recv):
        @pl.loop(1, n)
        def _(k):
            feat_copy(
                dst.at[me], dst.at[me], send.at[k], recv.at[me], (me + k) % n).wait_send()

    def hits(index_row, size):
        level = lax.broadcasted_iota(jnp.int32, (size, height), 0).astype(F32).astype(BF16)
        return level == index_row.astype(F32).astype(BF16)

    def high_hits(index_row):
        return hits(index_row >> LANE_BITS, high_size)

    def low_hits(index_row):
        return hits(index_row & (LANES - 1), LANES)

    one, zero = jnp.ones((), BF16), jnp.zeros((), BF16)

    loads[0].wait()
    pl.semaphore_wait(barrier, n - 1 + shards - 1)
    sends(idx_all, idx_ss, idx_rs)
    for load in loads[1:]:
        load.wait()
    iterate = lx[...]
    dual_local = dual[...]
    target = cons[...] - dual_local

    own = idx_all[me]
    labels_hl = lab[...].astype(F32).astype(BF16)
    targets = []
    for b in range(blocks):
        row = own[b:b + 1, :]
        low = jnp.where(low_hits(row), one, zero)
        high = jnp.where(high_hits(row), one, zero)
        oh_hi[b] = high
        oh_lo[b] = low
        picked = dot_nn(labels_hl, low)
        targets.append(jnp.sum(picked * high.astype(F32), axis=0, keepdims=True))
        data_t[b] = data[b].T

    def products(iterate):
        rounded = iterate.astype(BF16)
        return jnp.concatenate(
            [dot_nn(rounded, data_t[b])[b:b + 1] for b in range(blocks)], axis=0)

    def scatter(index, values):
        total = jnp.zeros((2 * high_size, LANES), F32)
        first, second = two_terms(values)
        first, second = first.astype(BF16), second.astype(BF16)
        for b in range(blocks):
            row = index[b:b + 1, :]
            mask = high_hits(row)
            low = jnp.where(low_hits(row), one, zero)
            spread = jnp.concatenate(
                [jnp.where(mask, first[b:b + 1, :], zero),
                 jnp.where(mask, second[b:b + 1, :], zero)], axis=0)
            total += dot_nt(spread, low)
        return total

    def newton_step(step, iterate):
        slots, slot_ss, slot_rs = p_all.at[step], p_ss.at[step], p_rs.at[step]
        slots[me] = products(iterate)
        sends(slots, slot_ss, slot_rs)

        def collect(k, total):
            @pl.when((step == 0) & (k > 0))
            def _():
                wait_from(idx_all, idx_ss, idx_rs, k)

            @pl.when(k > 0)
            def _():
                wait_from(slots, slot_ss, slot_rs, k)

            source = (me + n - k) % n
            return total + scatter(idx_all[source], slots[source])

        total = lax.fori_loop(0, n, collect, jnp.zeros((2 * high_size, LANES), F32))
        margins = total[:high_size] + total[high_size:]
        margins_two = jnp.concatenate(two_terms(margins), axis=0).astype(BF16)
        gradient = []
        for b in range(blocks):
            picked = dot_nn(margins_two, oh_lo[b])
            both = picked[:high_size] + picked[high_size:]
            margin = jnp.sum(both * oh_hi[b].astype(F32), axis=0, keepdims=True)
            prob = 1.0 / (1.0 + jnp.exp(-margin))
            weights = prob * (1.0 - prob)
            misfit = jnp.broadcast_to(prob - targets[b], (16, height))
            left = jnp.concatenate(
                [(data_t[b].astype(F32) * weights).astype(BF16), misfit.astype(BF16)], axis=0)
            made = dot_nn(left, data[b])
            hess[b] = made[:width]
            gradient.append(made[width:width + 1])
        gradient = jnp.concatenate(gradient, axis=0) + penalty * (iterate - target)

        def cg_step(_, state):
            delta, residual, direction, power = state
            turned = direction.T
            image = jnp.concatenate(
                [jnp.sum(hess[b] * turned[:, b:b + 1], axis=0, keepdims=True)
                 for b in range(blocks)], axis=0) + penalty * direction
            alpha = power / jnp.sum(direction * image, axis=1, keepdims=True)
            delta = delta + alpha * direction
            residual = residual - alpha * image
            power_next = jnp.sum(residual * residual, axis=1, keepdims=True)
            direction = residual + (power_next / power) * direction
            return delta, residual, direction, power_next

        power = jnp.sum(gradient * gradient, axis=1, keepdims=True)
        delta = lax.fori_loop(
            0, CG_STEPS, cg_step, (jnp.zeros_like(gradient), gradient, gradient, power))[0]
        return iterate - damping * delta

    iterate = lax.fori_loop(0, NEWTON_STEPS, newton_step, iterate)

    fin[shard, 0] = iterate + dual_local
    fin[shard, 1] = iterate

    def fin_copy(j, slot):
        return pltpu.make_async_remote_copy(
            src_ref=fin.at[shard], dst_ref=fin.at[slot],
            send_sem=fin_ss.at[j], recv_sem=fin_rs.at[slot],
            device_id=shard_id((shard + j) % shards), device_id_type=MESH)

    for j in range(1, shards):
        fin_copy(j, shard).start()
    for j in range(1, shards):
        fin_copy(j, (shard + shards - j) % shards).wait_recv()
    totals = fin[0, 0]
    for s in range(1, shards):
        totals += fin[s, 0]
    averaged = totals / F32(shards)
    size = jnp.maximum(jnp.abs(averaged) - threshold, 0.0)
    consensus = jnp.where(averaged > 0.0, size, -size)
    change = (consensus - cons[...]) ** 2
    primal = (fin[0, 1] - consensus) ** 2
    for s in range(1, shards):
        primal += (fin[s, 1] - consensus) ** 2
    nrm[me] = jnp.concatenate(
        [jnp.sum(primal, axis=0, keepdims=True), jnp.sum(change, axis=0, keepdims=True)], axis=0)
    sends(nrm, nrm_ss, nrm_rs)
    packed_out[0] = iterate
    packed_out[1] = dual_local + iterate - consensus
    packed_out[2] = consensus
    for j in range(1, shards):
        fin_copy(j, shard).wait_send()
    wait_sends(idx_all, idx_ss, idx_rs)
    for step in range(NEWTON_STEPS):
        wait_sends(p_all.at[step], p_ss.at[step], p_rs.at[step])

    @pl.loop(1, n)
    def _(k):
        wait_from(nrm, nrm_ss, nrm_rs, k)

    sums = jnp.sum(jnp.sum(nrm[...], axis=0), axis=1, keepdims=True)
    factor = lax.broadcasted_iota(jnp.int32, sums.shape, 0)
    scaled = jnp.where(factor == 0, sums, F32(shards) * sums)
    norms = jnp.sqrt(scaled) * jnp.where(factor == 0, 1.0, penalty)
    packed_out[3, :2] = jnp.broadcast_to(norms, (2, width))
    wait_sends(nrm, nrm_ss, nrm_rs)


def unpack(packed, sx_out, dn_out, co_out, norm_out):
    sx_out[0] = packed[0]
    dn_out[0] = packed[1]
    co_out[...] = packed[2]
    norm_out[0] = packed[3, 0, 0]
    norm_out[1] = packed[3, 1, 0]


def local(mesh, local_x, dual_var, consensus_old, blocks_data, row_index, labels):
    n, rows, cols = mesh.shape["feat"], mesh.shape["row"], mesh.shape["col"]
    shards = rows * cols
    _, blocks, height, width = blocks_data.shape
    samples = labels.shape[1]
    high_size = samples // LANES
    dma = pltpu.SemaphoreType.DMA
    vmem = pl.BlockSpec(memory_space=pltpu.VMEM)
    packed = pl.pallas_call(
        functools.partial(kernel, n, rows, cols),
        out_shape=jax.ShapeDtypeStruct((4, max(blocks, 2), width), F32),
        in_specs=[pl.BlockSpec(memory_space=pl.ANY)] * 6,
        out_specs=vmem,
        scratch_shapes=[
            pltpu.VMEM((blocks, width), F32),
            pltpu.VMEM((blocks, width), F32),
            pltpu.VMEM((blocks, width), F32),
            pltpu.VMEM((high_size, LANES), jnp.int32),
            pltpu.VMEM((blocks, height, width), BF16),
            pltpu.VMEM((blocks, width, height), BF16),
            pltpu.VMEM((blocks, width, width), F32),
            pltpu.VMEM((NEWTON_STEPS, n, blocks, height), F32),
            pltpu.VMEM((n, blocks, height), jnp.int32),
            pltpu.VMEM((shards, 2, blocks, width), F32),
            pltpu.VMEM((n, 2, width), F32),
            pltpu.VMEM((blocks, high_size, height), BF16),
            pltpu.VMEM((blocks, LANES, height), BF16),
            dma((6,)),
            dma((n,)), dma((n,)),
            dma((NEWTON_STEPS, n)), dma((NEWTON_STEPS, n)),
            dma((shards,)), dma((shards,)),
            dma((n,)), dma((n,)),
        ],
        compiler_params=pltpu.CompilerParams(
            collective_id=0, has_side_effects=True, vmem_limit_bytes=56 * 1024 * 1024),
        name="admm",
    )(local_x, dual_var, consensus_old, row_index, labels.reshape(high_size, LANES), blocks_data)
    return pl.pallas_call(
        unpack,
        out_shape=(
            jax.ShapeDtypeStruct(local_x.shape, F32),
            jax.ShapeDtypeStruct(local_x.shape, F32),
            jax.ShapeDtypeStruct(consensus_old.shape, F32),
            jax.ShapeDtypeStruct((2,), F32),
        ),
        in_specs=[vmem],
        out_specs=(vmem, vmem, vmem, pl.BlockSpec(memory_space=pltpu.SMEM)),
        name="unpack",
    )(packed)


def solution(mesh):
    placed = (
        P(("row", "col"), "feat", None),
        P(("row", "col"), "feat", None),
        P("feat", None),
        P(("row", "col"), "feat", None, None),
        P(("row", "col"), "feat", None),
        P(("row", "col"), None),
    )
    return jax.shard_map(
        functools.partial(local, mesh),
        mesh=mesh,
        in_specs=placed,
        out_specs=(
            P(("row", "col"), "feat", None),
            P(("row", "col"), "feat", None),
            P("feat", None),
            P(),
        ),
        check_vma=False,
    )
```
